32 devices in a mesh: sweep: 2 (over y), row: 4 (over x, core), col: 4 (over z).
Axes of the slice: x: 2, y: 2, z: 4, core: 2. Of those that a mesh axis runs over, the one named last changes fastest.
Arguments:
- tokens: bfloat16 [160, 4096], P(('sweep', 'col'), 'row'), parts along dimension 0, may hold values from -6 to 6
- w_gate: bfloat16 [4096, 14336], P('row', 'col'), may hold values from -0.09375 to 0.09375
- w_up: bfloat16 [4096, 14336], P('row', 'col'), may hold values from -0.09375 to 0.09375
- w_down: bfloat16 [14336, 4096], P('col', 'row'), may hold values from -0.046875 to 0.046875
- cotangent: bfloat16 [160, 4096], P(('sweep', 'col'), 'row'), parts along dimension 0, may hold values from -6 to 6
- step_rate: float32 [2], P('sweep'), parts along dimension 0, may hold values from 0.05 to 0.3
Outputs:
- out_rows: bfloat16 [160, 4096], P(('sweep', 'col'), 'row'), parts along dimension 0
- grad_in: bfloat16 [160, 4096], P(('sweep', 'col'), 'row'), parts along dimension 0
- step_gate: bfloat16 [8192, 14336], P(('sweep', 'row'), 'col'), parts along dimension 0
- step_up: bfloat16 [8192, 14336], P(('sweep', 'row'), 'col'), parts along dimension 0
- step_down: bfloat16 [28672, 4096], P(('sweep', 'col'), 'row'), parts along dimension 0
The draws below stay inside these ranges and needn't reach their ends.
There are 2 independent parts, one for each index of `sweep`. The reference program is written for one: setup_inputs(seed, part) draws one part's arguments, and reference() takes and returns one part's arrays. A program takes and returns all parts, laid end to end along the dimension named above; an argument that names none is the same for every part. Nothing has to cross between parts.
All inputs are finite; a program needn't handle non-finite values.
Results may differ from the reference program's by a relative error of at most 0.0049.
Values may be sent and summed in bfloat16 or wider, within the bound.
A program may use at most 128 MiB of HBM per device.

```python
import math
import jax
import jax.numpy as jnp

D = 4096
FF = 14336
TOKENS = 80


def levels(stream_key, shape, shards, low, high):
    gain = 1.0
    for dim, parts in shards:
        steps = jax.random.uniform(jax.random.fold_in(jax.random.fold_in(stream_key, 6), dim), (parts,), jnp.float32, low / len(shards), high / len(shards))
        gain = gain * jnp.repeat(jnp.exp(steps), shape[dim] // parts).reshape((-1,) + (1,) * (len(shape) - 1 - dim))
    return gain


def noise(stream_key, dims, deviation, limit, cuts=(), held_as=jnp.bfloat16):
    values = jax.random.normal(stream_key, dims, jnp.float32) * deviation
    if len(cuts) > 0:
        values = levels(stream_key, dims, cuts, -0.22, 0.18) * values
    return jnp.clip(values, min=-limit, max=limit).astype(held_as)


def setup_inputs(seed: int = 0, part: int = 0) -> dict:
    seeds = jax.random.split(jax.random.key(seed), 7)
    part_keys = jax.random.split(jax.random.fold_in(seeds[6], part), 7)
    return {
        "tokens": noise(part_keys[0], (TOKENS, D), 1.0, 6.0, ((0, 4), (1, 4))),
        "w_gate": noise(seeds[1], (D, FF), D ** -0.5, 0.09375, ((0, 4), (1, 4))),
        "w_up": noise(seeds[2], (D, FF), D ** -0.5, 0.09375, ((0, 4), (1, 4))),
        "w_down": noise(seeds[3], (FF, D), FF ** -0.5, 0.046875, ((0, 4), (1, 4))),
        "cotangent": noise(part_keys[4], (TOKENS, D), 1.0, 6.0, ((0, 4), (1, 4))),
        "step_rate": jnp.clip(jnp.exp(jax.random.uniform(part_keys[5], (1,), jnp.float32, math.log(0.05), math.log(0.3))), 0.05, 0.3),
    }


def reference(tokens, w_gate, w_up, w_down, cotangent, step_rate):
    gate_val = jnp.dot(tokens, w_gate, preferred_element_type=jnp.float32)
    up_val = jnp.dot(tokens, w_up, preferred_element_type=jnp.float32)
    gate_sig = jax.nn.sigmoid(gate_val)
    activation = gate_val * gate_sig
    hidden = (activation * up_val).astype(jnp.bfloat16)
    out_rows = (tokens.astype(jnp.float32) + jnp.dot(hidden, w_down, preferred_element_type=jnp.float32)).astype(jnp.bfloat16)
    back_hidden = jnp.dot(cotangent, w_down.T, preferred_element_type=jnp.float32)
    back_gate = (back_hidden * up_val * gate_sig * (1.0 + gate_val * (1.0 - gate_sig))).astype(jnp.bfloat16)
    back_up = (back_hidden * activation).astype(jnp.bfloat16)
    grad_total = cotangent.astype(jnp.float32) + jnp.dot(back_gate, w_gate.T, preferred_element_type=jnp.float32)
    grad_in = (grad_total + jnp.dot(back_up, w_up.T, preferred_element_type=jnp.float32)).astype(jnp.bfloat16)
    factor = -step_rate[0]
    step_gate = (factor * jnp.dot(tokens.T, back_gate, preferred_element_type=jnp.float32)).astype(jnp.bfloat16)
    step_up = (factor * jnp.dot(tokens.T, back_up, preferred_element_type=jnp.float32)).astype(jnp.bfloat16)
    step_down = (factor * jnp.dot(hidden.T, cotangent, preferred_element_type=jnp.float32)).astype(jnp.bfloat16)
    return out_rows, grad_in, step_gate, step_up, step_down
```

```python
import functools

import jax
import jax.numpy as jnp
from jax import lax
from jax.experimental import pallas as pl
from jax.experimental.pallas import tpu as pltpu
from jax.sharding import PartitionSpec as P

MESH = pl.DeviceIdType.MESH
VMEM_BYTES = 60 * 1024 * 1024


def contract(left, right, dims):
    return lax.dot_general(left, right, ((dims[:1], dims[1:]), ((), ())), preferred_element_type=jnp.float32)


def layer_kernel(
    n_row, n_col, chunks,
    tok_ref, cot_ref, wg_hbm, wu_hbm, wd_hbm,
    *refs,
):
    outs, scratch = refs[: 6 + n_col - 1], refs[6 + n_col - 1 :]
    tok_mat, cot_mat, hid_ref, bg_ref, bu_ref, own_ref = outs[:6]
    send_refs = outs[6:]
    (wg, wu, wd, gathered, stage, part, d2d, xs, xr, act, acc, zacc,
     wsem, zsend, zrecv, dsend, drecv, xsend, xrecv, asend, arecv) = scratch
    rows = tok_ref.shape[0]
    half = rows * n_col // 2
    width = wg.shape[2]
    n_x = n_row // 2
    row, col = lax.axis_index("row"), lax.axis_index("col")
    core, x = lax.rem(row, 2), row // 2
    other = 1 - core
    core_peer = {"row": x * 2 + other}

    def weight_copies(k):
        static = isinstance(k, int) or chunks == 1
        start = (0 if chunks == 1 else k * width) if static else pl.multiple_of(k * width, width)
        cut = pl.ds(start, width)
        return (
            pltpu.make_async_copy(wg_hbm.at[:, cut], wg.at[k], wsem.at[0, k]),
            pltpu.make_async_copy(wu_hbm.at[:, cut], wu.at[k], wsem.at[1, k]),
            pltpu.make_async_copy(wd_hbm.at[cut, :], wd.at[k], wsem.at[2, k]),
        )

    for k in range(chunks):
        for copy in weight_copies(k):
            copy.start()

    barrier = pltpu.get_barrier_semaphore()
    peers = [core_peer]
    peers += [{"row": lax.rem(x + o, n_x) * 2 + core} for o in range(1, n_x)]
    peers += [{"col": lax.rem(col + o, n_col)} for o in range(1, n_col)]
    for peer in peers:
        pl.semaphore_signal(barrier, inc=1, device_id=peer, device_id_type=MESH)
    pl.semaphore_wait(barrier, len(peers))

    def gather_copy(t, o, slot):
        return pltpu.make_async_remote_copy(
            src_ref=(tok_ref, cot_ref)[t], dst_ref=gathered.at[t, slot],
            send_sem=zsend.at[t, o], recv_sem=zrecv.at[t, o],
            device_id={"col": lax.rem(col + o, n_col)}, device_id_type=MESH,
        )

    for t in range(2):
        for o in range(1, n_col):
            gather_copy(t, o, col).start()
    gathered[0, col] = tok_ref[...]
    gathered[1, col] = cot_ref[...]
    for t in range(2):
        for o in range(1, n_col):
            gather_copy(t, o, lax.rem(col + n_col - o, n_col)).wait_recv()
        for j in range(n_col):
            stage[j * rows : (j + 1) * rows, :] = gathered[t, j].astype(jnp.float32)
        (tok_mat, cot_mat)[t][...] = stage[...].astype(jnp.bfloat16)

    def core_copy(k):
        return pltpu.make_async_remote_copy(
            src_ref=part.at[k, other], dst_ref=d2d.at[k],
            send_sem=dsend.at[k], recv_sem=drecv.at[k],
            device_id=core_peer, device_id_type=MESH,
        )

    def x_copy(k, o):
        return pltpu.make_async_remote_copy(
            src_ref=xs.at[k], dst_ref=xr.at[k, o - 1],
            send_sem=xsend.at[k, o - 1], recv_sem=xrecv.at[k, o - 1],
            device_id={"row": lax.rem(x + o, n_x) * 2 + core}, device_id_type=MESH,
        )

    def act_copy(k, which):
        return pltpu.make_async_remote_copy(
            src_ref=act.at[k, which], dst_ref=act.at[k, which],
            send_sem=asend.at[k], recv_sem=arecv.at[k],
            device_id=core_peer, device_id_type=MESH,
        )

    def first_loop(k, carry):
        @pl.when(k < chunks)
        def _():
            for copy in weight_copies(k):
                copy.wait()
            sums = (
                contract(tok_mat[...], wg[k], (1, 0)),
                contract(tok_mat[...], wu[k], (1, 0)),
                contract(cot_mat[...], wd[k], (1, 1)),
            )
            for m in range(3):
                for h in range(2):
                    part[k, h, m * half : (m + 1) * half, :] = sums[m][h * half : (h + 1) * half]
            core_copy(k).start()

        @pl.when(k > 0)
        def _():
            last = k - 1
            core_copy(last).wait_recv()
            total = part[last, core] + d2d[last]
            d2d[last] = total
            xs[last] = total.astype(jnp.bfloat16)
            for o in range(1, n_x):
                x_copy(last, o).start()

        return carry

    lax.fori_loop(0, chunks + 1, first_loop, 0)

    acc[...] = jnp.zeros_like(acc)

    def second_loop(k, carry):
        @pl.when(k < chunks)
        def _():
            total = d2d[k]
            for o in range(1, n_x):
                x_copy(k, o).wait_recv()
                total = total + xr[k, o - 1].astype(jnp.float32)
            gate_val, up_val, back_hidden = total[:half], total[half : 2 * half], total[2 * half :]
            gate_sig = jax.nn.sigmoid(gate_val)
            activation = gate_val * gate_sig
            hidden = activation * up_val
            back_gate = back_hidden * up_val * gate_sig * (1.0 + gate_val * (1.0 - gate_sig))
            back_up = back_hidden * activation
            act[k, core] = jnp.concatenate([hidden, back_gate, back_up], axis=0).astype(jnp.bfloat16)
            act_copy(k, core).start()

        @pl.when(k > 0)
        def _():
            last = k - 1
            act_copy(last, other).wait_recv()
            low = act[last, 0].astype(jnp.float32)
            high = act[last, 1].astype(jnp.float32)
            picked = [
                jnp.concatenate(
                    [low[m * half : (m + 1) * half], high[m * half : (m + 1) * half]], axis=0
                ).astype(jnp.bfloat16)
                for m in range(3)
            ]
            hid_ref[last], bg_ref[last], bu_ref[last] = picked
            acc[0] += contract(picked[0], wd[last], (1, 0))
            acc[1] += contract(picked[1], wg[last], (1, 1)) + contract(picked[2], wu[last], (1, 1))

        return carry

    lax.fori_loop(0, chunks + 1, second_loop, 0)

    for t in range(2):
        for j in range(n_col):
            zacc[t, j] = acc[t, j * rows : (j + 1) * rows, :]
    own_ref[...] = zacc[:, col]
    for o in range(1, n_col):
        send_refs[o - 1][...] = zacc[:, lax.rem(col + o, n_col)].astype(jnp.bfloat16)

    for t in range(2):
        for o in range(1, n_col):
            gather_copy(t, o, col).wait_send()

    def drain(k, carry):
        core_copy(k).wait_send()
        for o in range(1, n_x):
            x_copy(k, o).wait_send()
        act_copy(k, core).wait_send()
        return carry

    lax.fori_loop(0, chunks, drain, 0)


def layer_call(n_row, n_col, width, tokens, cotangent, w_gate, w_up, w_down):
    rows, depth = tokens.shape
    hidden_width = w_gate.shape[1]
    chunks = hidden_width // width
    total = rows * n_col
    half3 = 3 * total // 2
    n_x = n_row // 2
    bf16, f32 = jnp.bfloat16, jnp.float32
    vmem = pl.BlockSpec(memory_space=pltpu.VMEM)
    hbm = pl.BlockSpec(memory_space=pl.ANY)
    out_shape = [jax.ShapeDtypeStruct((total, depth), bf16)] * 2
    out_shape += [jax.ShapeDtypeStruct((chunks, total, width), bf16)] * 3
    out_shape += [jax.ShapeDtypeStruct((2, rows, depth), f32)]
    out_shape += [jax.ShapeDtypeStruct((2, rows, depth), bf16)] * (n_col - 1)
    sem = pltpu.SemaphoreType.DMA
    return pl.pallas_call(
        functools.partial(layer_kernel, n_row, n_col, chunks),
        out_shape=out_shape,
        in_specs=[vmem, vmem, hbm, hbm, hbm],
        out_specs=[vmem] * len(out_shape),
        scratch_shapes=[
            pltpu.VMEM((chunks, depth, width), bf16),
            pltpu.VMEM((chunks, depth, width), bf16),
            pltpu.VMEM((chunks, width, depth), bf16),
            pltpu.VMEM((2, n_col, rows, depth), bf16),
            pltpu.VMEM((total, depth), f32),
            pltpu.VMEM((chunks, 2, half3, width), f32),
            pltpu.VMEM((chunks, half3, width), f32),
            pltpu.VMEM((chunks, half3, width), bf16),
            pltpu.VMEM((chunks, max(n_x - 1, 1), half3, width), bf16),
            pltpu.VMEM((chunks, 2, half3, width), bf16),
            pltpu.VMEM((2, total, depth), f32),
            pltpu.VMEM((2, n_col, rows, depth), f32),
            sem((3, chunks)),
            sem((2, n_col)),
            sem((2, n_col)),
            sem((chunks,)),
            sem((chunks,)),
            sem((chunks, max(n_x - 1, 1))),
            sem((chunks, max(n_x - 1, 1))),
            sem((chunks,)),
            sem((chunks,)),
        ],
        compiler_params=pltpu.CompilerParams(
            collective_id=0, has_side_effects=True, vmem_limit_bytes=VMEM_BYTES
        ),
        cost_estimate=pl.CostEstimate(
            flops=12 * total * depth * hidden_width,
            bytes_accessed=6 * depth * hidden_width,
            transcendentals=total * hidden_width,
        ),
    )(tokens, cotangent, w_gate, w_up, w_down)


def step_kernel(rate_ref, tok_ref, cot_ref, hid_ref, bg_ref, bu_ref, sg_ref, su_ref, sd_ref):
    factor = -rate_ref[0]
    sg_ref[...] = (factor * contract(tok_ref[...], bg_ref[0], (0, 0))).astype(jnp.bfloat16)
    su_ref[...] = (factor * contract(tok_ref[...], bu_ref[0], (0, 0))).astype(jnp.bfloat16)
    sd_ref[...] = (factor * contract(hid_ref[0], cot_ref[...], (0, 0))).astype(jnp.bfloat16)


def step_call(step_rate, tok_mat, cot_mat, hid, bg, bu):
    chunks, total, width = hid.shape
    depth = tok_mat.shape[1]
    whole = pl.BlockSpec((total, depth), lambda k: (0, 0))
    piece = pl.BlockSpec((1, total, width), lambda k: (k, 0, 0))
    wide = pl.BlockSpec((depth, width), lambda k: (0, k))
    tall = pl.BlockSpec((width, depth), lambda k: (k, 0))
    bf16 = jnp.bfloat16
    return pl.pallas_call(
        step_kernel,
        grid=(chunks,),
        out_shape=[
            jax.ShapeDtypeStruct((depth, chunks * width), bf16),
            jax.ShapeDtypeStruct((depth, chunks * width), bf16),
            jax.ShapeDtypeStruct((chunks * width, depth), bf16),
        ],
        in_specs=[pl.BlockSpec(memory_space=pltpu.SMEM), whole, whole, piece, piece, piece],
        out_specs=[wide, wide, tall],
        compiler_params=pltpu.CompilerParams(vmem_limit_bytes=VMEM_BYTES // 2),
        cost_estimate=pl.CostEstimate(
            flops=6 * total * depth * chunks * width,
            bytes_accessed=6 * depth * chunks * width,
            transcendentals=0,
        ),
    )(step_rate, tok_mat, cot_mat, hid, bg, bu)


def local(n_row, n_col, tokens, w_gate, w_up, w_down, cotangent, step_rate):
    hidden_width = w_gate.shape[1]
    width = 512 if hidden_width % 512 == 0 else hidden_width
    tok_mat, cot_mat, hid, bg, bu, own, *sends = layer_call(
        n_row, n_col, width, tokens, cotangent, w_gate, w_up, w_down
    )
    arrived = [
        lax.ppermute(block, "col", [(i, (i + o) % n_col) for i in range(n_col)])
        for o, block in enumerate(sends, 1)
    ]
    step_gate, step_up, step_down = step_call(step_rate, tok_mat, cot_mat, hid, bg, bu)
    sums = own
    for block in arrived:
        sums = sums + block.astype(jnp.float32)
    out_rows = (tokens.astype(jnp.float32) + sums[0]).astype(jnp.bfloat16)
    grad_in = (cotangent.astype(jnp.float32) + sums[1]).astype(jnp.bfloat16)
    return (out_rows, grad_in, step_gate, step_up, step_down)


def solution(mesh):
    in_specs = (
        P(("sweep", "col"), "row"),
        P("row", "col"),
        P("row", "col"),
        P("col", "row"),
        P(("sweep", "col"), "row"),
        P("sweep"),
    )
    out_specs = (
        P(("sweep", "col"), "row"),
        P(("sweep", "col"), "row"),
        P(("sweep", "row"), "col"),
        P(("sweep", "row"), "col"),
        P(("sweep", "col"), "row"),
    )
    body = functools.partial(local, mesh.shape["row"], mesh.shape["col"])
    return jax.shard_map(body, mesh=mesh, in_specs=in_specs, out_specs=out_specs, check_vma=False)
```

```python
import functools

import jax
import jax.numpy as jnp
from jax import lax
from jax.experimental import pallas as pl
from jax.experimental.pallas import tpu as pltpu
from jax.sharding import PartitionSpec as P

MESH = pl.DeviceIdType.MESH
LAYER_VMEM = 49 * 1024 * 1024
STEP_VMEM = 30 * 1024 * 1024


def contract(left, right, dims):
    return lax.dot_general(left, right, ((dims[:1], dims[1:]), ((), ())), preferred_element_type=jnp.float32)


def layer_kernel(
    n_row, n_col, chunks,
    tok_ref, cot_ref, wg_hbm, wu_hbm, wd_hbm,
    *refs,
):
    outs, scratch = refs[: 6 + n_col - 1], refs[6 + n_col - 1 :]
    tok_mat, cot_mat, hid_ref, bg_ref, bu_ref, own_ref = outs[:6]
    send_refs = outs[6:]
    (wg, wu, wd, gathered, stage, part, d2d, xs, xr, bpart, bd2d, bxs, bxr, act, bact, acc, zacc,
     wsem, zsend, zrecv, dsem, asem, xsend, xrecv) = scratch
    rows = tok_ref.shape[0]
    half = rows * n_col // 2
    width = wg.shape[2]
    n_x = n_row // 2
    row, col = lax.axis_index("row"), lax.axis_index("col")
    core, x = lax.rem(row, 2), row // 2
    other = 1 - core
    core_peer = {"row": x * 2 + other}

    def weight_copy(m, k):
        static = isinstance(k, int) or chunks == 1
        start = (0 if chunks == 1 else k * width) if static else pl.multiple_of(k * width, width)
        cut = pl.ds(start, width)
        source = (wg_hbm, wu_hbm, wd_hbm)[m]
        return pltpu.make_async_copy(
            source.at[cut, :] if m == 2 else source.at[:, cut], (wg, wu, wd)[m].at[k], wsem.at[m, k]
        )

    for k in range(chunks):
        weight_copy(0, k).start()
        weight_copy(1, k).start()
    for k in range(chunks):
        weight_copy(2, k).start()

    barrier = pltpu.get_barrier_semaphore()
    peers = [core_peer]
    peers += [{"row": lax.rem(x + o, n_x) * 2 + core} for o in range(1, n_x)]
    peers += [{"col": lax.rem(col + o, n_col)} for o in range(1, n_col)]
    for peer in peers:
        pl.semaphore_signal(barrier, inc=1, device_id=peer, device_id_type=MESH)
    pl.semaphore_wait(barrier, len(peers))

    def gather_copy(t, o, slot):
        return pltpu.make_async_remote_copy(
            src_ref=(tok_ref, cot_ref)[t], dst_ref=gathered.at[t, slot],
            send_sem=zsend.at[t, o], recv_sem=zrecv.at[t, o],
            device_id={"col": lax.rem(col + o, n_col)}, device_id_type=MESH,
        )

    for t in range(2):
        for o in range(1, n_col):
            gather_copy(t, o, col).start()
    gathered[0, col] = tok_ref[...]
    gathered[1, col] = cot_ref[...]

    def assemble(t):
        for o in range(1, n_col):
            gather_copy(t, o, lax.rem(col + n_col - o, n_col)).wait_recv()
        for j in range(n_col):
            stage[j * rows : (j + 1) * rows, :] = gathered[t, j].astype(jnp.float32)
        (tok_mat, cot_mat)[t][...] = stage[...].astype(jnp.bfloat16)

    sums_of = (part, bpart)
    landed_of = (d2d, bd2d)
    xs_of = (xs, bxs)
    xr_of = (xr, bxr)
    act_of = (act, bact)

    def core_copy(t, k):
        return pltpu.make_async_remote_copy(
            src_ref=sums_of[t].at[k, other], dst_ref=landed_of[t].at[k],
            send_sem=dsem.at[0, t, k], recv_sem=dsem.at[1, t, k],
            device_id=core_peer, device_id_type=MESH,
        )

    def x_copy(t, k, o):
        return pltpu.make_async_remote_copy(
            src_ref=xs_of[t].at[k], dst_ref=xr_of[t].at[k, o - 1],
            send_sem=xsend.at[t, k, o - 1], recv_sem=xrecv.at[t, k, o - 1],
            device_id={"row": lax.rem(x + o, n_x) * 2 + core}, device_id_type=MESH,
        )

    def act_copy(t, k, which):
        return pltpu.make_async_remote_copy(
            src_ref=act_of[t].at[k, which], dst_ref=act_of[t].at[k, which],
            send_sem=asem.at[0, t, k], recv_sem=asem.at[1, t, k],
            device_id=core_peer, device_id_type=MESH,
        )

    def share(t, k):
        core_copy(t, k).wait_recv()
        total = sums_of[t][k, core] + landed_of[t][k]
        landed_of[t][k] = total
        xs_of[t][k] = total.astype(jnp.bfloat16)
        for o in range(1, n_x):
            x_copy(t, k, o).start()

    def total_of(t, k):
        total = landed_of[t][k]
        for o in range(1, n_x):
            x_copy(t, k, o).wait_recv()
            total = total + xr_of[t][k, o - 1].astype(jnp.float32)
        return total

    def both(t, k, m):
        return jnp.concatenate(
            [act_of[t][k, h, m * half : (m + 1) * half, :].astype(jnp.float32) for h in range(2)], axis=0
        ).astype(jnp.bfloat16)

    def staged(begin, finish):
        def step(k, carry):
            @pl.when(k < chunks)
            def _():
                begin(k)

            @pl.when(k > 0)
            def _():
                finish(k - 1)

            return carry

        lax.fori_loop(0, chunks + 1, step, 0)

    def forward_sums(k):
        weight_copy(0, k).wait()
        weight_copy(1, k).wait()
        for m, w in enumerate((wg, wu)):
            sums = contract(tok_mat[...], w[k], (1, 0))
            for h in range(2):
                part[k, h, m * half : (m + 1) * half, :] = sums[h * half : (h + 1) * half]
        core_copy(0, k).start()

    def backward_sums(k):
        weight_copy(2, k).wait()
        sums = contract(cot_mat[...], wd[k], (1, 1))
        for h in range(2):
            bpart[k, h] = sums[h * half : (h + 1) * half]
        core_copy(1, k).start()

    def forward_act(k):
        total = total_of(0, k)
        d2d[k] = total
        gate_val, up_val = total[:half], total[half:]
        act[k, core] = (gate_val * jax.nn.sigmoid(gate_val) * up_val).astype(jnp.bfloat16)
        act_copy(0, k, core).start()

    def forward_out(k):
        act_copy(0, k, other).wait_recv()
        hidden = both(0, k, 0)
        hid_ref[k] = hidden
        acc[0] += contract(hidden, wd[k], (1, 0))

    def backward_act(k):
        back_hidden = total_of(1, k)
        gate_val, up_val = d2d[k, :half], d2d[k, half:]
        gate_sig = jax.nn.sigmoid(gate_val)
        back_gate = back_hidden * up_val * gate_sig * (1.0 + gate_val * (1.0 - gate_sig))
        back_up = back_hidden * (gate_val * gate_sig)
        bact[k, core] = jnp.concatenate([back_gate, back_up], axis=0).astype(jnp.bfloat16)
        act_copy(1, k, core).start()

    def backward_out(k):
        act_copy(1, k, other).wait_recv()
        back_gate, back_up = both(1, k, 0), both(1, k, 1)
        bg_ref[k], bu_ref[k] = back_gate, back_up
        acc[1] += contract(back_gate, wg[k], (1, 1)) + contract(back_up, wu[k], (1, 1))

    acc[...] = jnp.zeros_like(acc)
    assemble(0)
    staged(forward_sums, lambda k: share(0, k))
    assemble(1)
    staged(backward_sums, lambda k: share(1, k))
    staged(forward_act, forward_out)
    staged(backward_act, backward_out)

    for t in range(2):
        for j in range(n_col):
            zacc[t, j] = acc[t, j * rows : (j + 1) * rows, :]
    own_ref[...] = zacc[:, col]
    for o in range(1, n_col):
        send_refs[o - 1][...] = zacc[:, lax.rem(col + o, n_col)].astype(jnp.bfloat16)

    for t in range(2):
        for o in range(1, n_col):
            gather_copy(t, o, col).wait_send()

    def drain(k, carry):
        for t in range(2):
            core_copy(t, k).wait_send()
            for o in range(1, n_x):
                x_copy(t, k, o).wait_send()
            act_copy(t, k, core).wait_send()
        return carry

    lax.fori_loop(0, chunks, drain, 0)


def layer_call(n_row, n_col, width, tokens, cotangent, w_gate, w_up, w_down):
    rows, depth = tokens.shape
    hidden_width = w_gate.shape[1]
    chunks = hidden_width // width
    total = rows * n_col
    half = total // 2
    others = max(n_row // 2 - 1, 1)
    bf16, f32 = jnp.bfloat16, jnp.float32
    vmem = pl.BlockSpec(memory_space=pltpu.VMEM)
    hbm = pl.BlockSpec(memory_space=pl.ANY)
    out_shape = [jax.ShapeDtypeStruct((total, depth), bf16)] * 2
    out_shape += [jax.ShapeDtypeStruct((chunks, total, width), bf16)] * 3
    out_shape += [jax.ShapeDtypeStruct((2, rows, depth), f32)]
    out_shape += [jax.ShapeDtypeStruct((2, rows, depth), bf16)] * (n_col - 1)
    sem = pltpu.SemaphoreType.DMA
    return pl.pallas_call(
        functools.partial(layer_kernel, n_row, n_col, chunks),
        out_shape=out_shape,
        in_specs=[vmem, vmem, hbm, hbm, hbm],
        out_specs=[vmem] * len(out_shape),
        scratch_shapes=[
            pltpu.VMEM((chunks, depth, width), bf16),
            pltpu.VMEM((chunks, depth, width), bf16),
            pltpu.VMEM((chunks, width, depth), bf16),
            pltpu.VMEM((2, n_col, rows, depth), bf16),
            pltpu.VMEM((total, depth), f32),
            pltpu.VMEM((chunks, 2, total, width), f32),
            pltpu.VMEM((chunks, total, width), f32),
            pltpu.VMEM((chunks, total, width), bf16),
            pltpu.VMEM((chunks, others, total, width), bf16),
            pltpu.VMEM((chunks, 2, half, width), f32),
            pltpu.VMEM((chunks, half, width), f32),
            pltpu.VMEM((chunks, half, width), bf16),
            pltpu.VMEM((chunks, others, half, width), bf16),
            pltpu.VMEM((chunks, 2, half, width), bf16),
            pltpu.VMEM((chunks, 2, total, width), bf16),
            pltpu.VMEM((2, total, depth), f32),
            pltpu.VMEM((2, n_col, rows, depth), f32),
            sem((3, chunks)),
            sem((2, n_col)),
            sem((2, n_col)),
            sem((2, 2, chunks)),
            sem((2, 2, chunks)),
            sem((2, chunks, others)),
            sem((2, chunks, others)),
        ],
        compiler_params=pltpu.CompilerParams(
            collective_id=0, has_side_effects=True, vmem_limit_bytes=LAYER_VMEM
        ),
        cost_estimate=pl.CostEstimate(
            flops=12 * total * depth * hidden_width,
            bytes_accessed=6 * depth * hidden_width,
            transcendentals=total * hidden_width,
        ),
    )(tokens, cotangent, w_gate, w_up, w_down)


def step_kernel(rate_ref, tok_ref, cot_ref, hid_ref, bg_ref, bu_ref, sg_ref, su_ref, sd_ref):
    factor = -rate_ref[0]
    sg_ref[...] = (factor * contract(tok_ref[...], bg_ref[0], (0, 0))).astype(jnp.bfloat16)
    su_ref[...] = (factor * contract(tok_ref[...], bu_ref[0], (0, 0))).astype(jnp.bfloat16)
    sd_ref[...] = (factor * contract(hid_ref[0], cot_ref[...], (0, 0))).astype(jnp.bfloat16)


def step_call(step_rate, tok_mat, cot_mat, hid, bg, bu):
    chunks, total, width = hid.shape
    depth = tok_mat.shape[1]
    whole = pl.BlockSpec((total, depth), lambda k: (0, 0))
    piece = pl.BlockSpec((1, total, width), lambda k: (k, 0, 0))
    wide = pl.BlockSpec((depth, width), lambda k: (0, k))
    tall = pl.BlockSpec((width, depth), lambda k: (k, 0))
    bf16 = jnp.bfloat16
    return pl.pallas_call(
        step_kernel,
        grid=(chunks,),
        out_shape=[
            jax.ShapeDtypeStruct((depth, chunks * width), bf16),
            jax.ShapeDtypeStruct((depth, chunks * width), bf16),
            jax.ShapeDtypeStruct((chunks * width, depth), bf16),
        ],
        in_specs=[pl.BlockSpec(memory_space=pltpu.SMEM), whole, whole, piece, piece, piece],
        out_specs=[wide, wide, tall],
        compiler_params=pltpu.CompilerParams(vmem_limit_bytes=STEP_VMEM),
        cost_estimate=pl.CostEstimate(
            flops=6 * total * depth * chunks * width,
            bytes_accessed=6 * depth * chunks * width,
            transcendentals=0,
        ),
    )(step_rate, tok_mat, cot_mat, hid, bg, bu)


def local(n_row, n_col, tokens, w_gate, w_up, w_down, cotangent, step_rate):
    hidden_width = w_gate.shape[1]
    width = 512 if hidden_width % 512 == 0 else hidden_width
    tok_mat, cot_mat, hid, bg, bu, own, *sends = layer_call(
        n_row, n_col, width, tokens, cotangent, w_gate, w_up, w_down
    )
    arrived = [
        lax.ppermute(block, "col", [(i, (i + o) % n_col) for i in range(n_col)])
        for o, block in enumerate(sends, 1)
    ]
    step_gate, step_up, step_down = step_call(step_rate, tok_mat, cot_mat, hid, bg, bu)
    finished = []
    for t, kept in enumerate((tokens, cotangent)):
        sums = own[t]
        for block in arrived:
            sums = sums + block[t].astype(jnp.float32)
        finished.append((kept.astype(jnp.float32) + sums).astype(jnp.bfloat16))
    out_rows, grad_in = finished
    return (out_rows, grad_in, step_gate, step_up, step_down)


def solution(mesh):
    in_specs = (
        P(("sweep", "col"), "row"),
        P("row", "col"),
        P("row", "col"),
        P("col", "row"),
        P(("sweep", "col"), "row"),
        P("sweep"),
    )
    out_specs = (
        P(("sweep", "col"), "row"),
        P(("sweep", "col"), "row"),
        P(("sweep", "row"), "col"),
        P(("sweep", "row"), "col"),
        P(("sweep", "col"), "row"),
    )
    body = functools.partial(local, mesh.shape["row"], mesh.shape["col"])
    return jax.shard_map(body, mesh=mesh, in_specs=in_specs, out_specs=out_specs, check_vma=False)
```
